32 devices in a mesh: gz: 2 (over x), row: 4 (over y, core), col: 4 (over z).
Axes of the slice: x: 2, y: 2, z: 4, core: 2. Of those that a mesh axis runs over, the one named last changes fastest.
Arguments:
- sections: bfloat16 [4, 2048, 2048], P('gz', 'row', 'col'), may hold values from -6 to 6
- priors: int32 [2, 4, 8, 8], P(None, 'gz', 'row', 'col'), may hold values from -64 to 64
- row_order: int32 [8], replicated, may hold values from 0 to 7, each once
Outputs:
- mesh_flows: float32 [8, 64], P('row')
The draws below stay inside these ranges and needn't reach their ends.
Inputs may be any that keep to these rules, and one draw needn't show every extreme that they name: A permutation of the patch rows: mesh row m holds patch row row_order[m].
All inputs are finite; a program needn't handle non-finite values.
Results may differ from the reference program's by a relative error of at most 0.0003.
Values may be sent and summed in bfloat16 or wider, within the bound.
A program may use at most 64 MiB of HBM per device.

```python
import math
import jax
import jax.numpy as jnp
from jax import lax

PATCH = 512
STRIDE = 256
LAGS = 128
MAXOFF = 64
HALO = 256
SECTIONS = 4
HEIGHT = 2048
WIDTH = 2048
GRID_R = 8
GRID_C = 8


def shared_shifts(key):
    shift_key = jax.random.fold_in(key, 4242)
    reach = MAXOFF // 8
    starts = jax.random.randint(jax.random.fold_in(shift_key, 1), (2, SECTIONS), -reach, reach + 1)
    slopes = jax.random.randint(jax.random.fold_in(shift_key, 2), (2, SECTIONS), -reach, reach + 1)
    return (starts, slopes)


def moved_by(starts, slopes, coords, extent):
    return starts[:, None] + slopes[:, None] * coords[None, :] // extent


def draw_sections(key, part):
    starts, slopes = shared_shifts(key)
    rows_all = jnp.arange(HEIGHT, dtype=jnp.int32)
    cols_all = jnp.arange(WIDTH, dtype=jnp.int32)
    row_shift = moved_by(starts[0], slopes[0], rows_all, HEIGHT)
    col_shift = moved_by(starts[1], slopes[1], cols_all, WIDTH)
    margin = MAXOFF
    texture_key = jax.random.fold_in(key, 11)
    noise_key = jax.random.fold_in(key, 12)
    texture = jax.random.normal(texture_key, (HEIGHT + 2 * margin, WIDTH + 2 * margin), jnp.float32)
    noise = jax.random.normal(noise_key, (SECTIONS, HEIGHT, WIDTH), jnp.float32)
    signal_weight = 0.9
    noise_weight = 0.45
    level = 1.0
    row_index = rows_all[None, :] - row_shift + margin
    col_index = cols_all[None, :] - col_shift + margin

    def one_section(row_pick, col_pick):
        return jnp.take(jnp.take(texture, row_pick, axis=0), col_pick, axis=1)
    moved = jax.vmap(one_section)(row_index, col_index)
    result = level * (signal_weight * moved + noise_weight * noise)
    return jnp.clip(result, -6.0, 6.0).astype(jnp.bfloat16)


def draw_priors(key, part):
    starts, slopes = shared_shifts(key)
    center_gap = PATCH // 2 - HALO // 2
    row_centers = jnp.clip(jnp.arange(GRID_R, dtype=jnp.int32) * STRIDE + center_gap, 0, HEIGHT - 1)
    col_centers = jnp.clip(jnp.arange(GRID_C, dtype=jnp.int32) * STRIDE + center_gap, 0, WIDTH - 1)
    row_shift = moved_by(starts[0], slopes[0], row_centers, HEIGHT)
    col_shift = moved_by(starts[1], slopes[1], col_centers, WIDTH)
    row_lag = jnp.roll(row_shift, -1, axis=0) - row_shift
    col_lag = jnp.roll(col_shift, -1, axis=0) - col_shift
    slack = MAXOFF // 2
    jitter = jax.random.randint(jax.random.fold_in(key, 13), (2, SECTIONS, GRID_R, GRID_C), -slack, slack + 1)
    row_prior = row_lag[:, :, None] + jitter[0]
    col_prior = col_lag[:, None, :] + jitter[1]
    result = jnp.clip(jnp.stack([row_prior, col_prior], axis=0), -MAXOFF, MAXOFF)
    result = result.at[0, 0, 0, 0].set(MAXOFF)
    result = result.at[0, SECTIONS - 1, 0, 0].set(-MAXOFF)
    result = result.at[1, 0, 0, 0].set(-MAXOFF)
    result = result.at[1, SECTIONS - 1, 0, 0].set(MAXOFF)
    return result.astype(jnp.int32)


def setup_inputs(seed: int = 0) -> dict:
    splits = jax.random.split(jax.random.key(seed), 4)
    sections = draw_sections(jax.random.fold_in(splits[3], 71), 0)
    priors = draw_priors(jax.random.fold_in(splits[3], 71), 0)
    row_order = jax.random.permutation(splits[2], GRID_R).astype(jnp.int32)
    return dict(sections=sections, priors=priors, row_order=row_order)


def dft_tables(length):
    frequencies = jnp.arange(length, dtype=jnp.int32)
    angles = jnp.mod(frequencies[:, None] * frequencies[None, :], length).astype(jnp.float32) * (2.0 * math.pi / length)
    cosine = jnp.cos(angles)
    sine_part = jnp.sin(angles)
    minus_table = jnp.concatenate([cosine, -sine_part], axis=1).astype(jnp.bfloat16)
    plus_table = jnp.concatenate([cosine, sine_part], axis=1).astype(jnp.bfloat16)
    return minus_table, plus_table


def spectra_of(patches, minus_table, plus_table):
    length = patches.shape[-1]
    row_pass = jnp.einsum('nxy,yk->nxk', patches.astype(jnp.float32), minus_table.astype(jnp.float32)).astype(jnp.bfloat16)
    real_rows = row_pass[:, :, :length]
    imag_rows = row_pass[:, :, length:]
    upper_stack = jnp.concatenate([real_rows, imag_rows], axis=1).astype(jnp.float32)
    lower_stack = jnp.concatenate([imag_rows, real_rows], axis=1).astype(jnp.float32)
    spec_real = jnp.einsum('kx,nxm->nkm', plus_table.astype(jnp.float32), upper_stack) / length
    spec_imag = jnp.einsum('kx,nxm->nkm', minus_table.astype(jnp.float32), lower_stack) / length
    return jnp.stack([spec_real, spec_imag], axis=1).astype(jnp.bfloat16)


def lag_angles(offsets, length):
    frequencies = jnp.arange(length, dtype=jnp.int32)
    shifts = offsets[:, None] + jnp.arange(LAGS, dtype=jnp.int32)[None, :] - LAGS // 2
    angles = jnp.mod(shifts[:, :, None] * frequencies[None, None, :], length).astype(jnp.float32) * (2.0 * math.pi / length)
    return jnp.cos(angles), jnp.sin(angles)


def flows_of(first_spec, second_spec, offsets):
    length = first_spec.shape[-1]
    first_real = first_spec[:, 0].astype(jnp.float32)
    first_imag = first_spec[:, 1].astype(jnp.float32)
    second_real = second_spec[:, 0].astype(jnp.float32)
    second_imag = second_spec[:, 1].astype(jnp.float32)
    prod_real = (first_real * second_real + first_imag * second_imag).astype(jnp.bfloat16)
    prod_imag = (first_real * second_imag - first_imag * second_real).astype(jnp.bfloat16)
    row_cosine, row_sine = lag_angles(offsets[0], length)
    column_cosine, column_sine = lag_angles(offsets[1], length)
    products = jnp.concatenate([prod_real, prod_imag], axis=2).astype(jnp.float32)
    column_real = jnp.concatenate([column_cosine, -column_sine], axis=2).astype(jnp.bfloat16).astype(jnp.float32)
    column_imag = jnp.concatenate([column_sine, column_cosine], axis=2).astype(jnp.bfloat16).astype(jnp.float32)
    half_real = jnp.einsum('nkl,nul->nku', products, column_real).astype(jnp.bfloat16)
    half_imag = jnp.einsum('nkl,nul->nku', products, column_imag).astype(jnp.bfloat16)
    row_table = jnp.concatenate([row_cosine, -row_sine], axis=2).astype(jnp.bfloat16).astype(jnp.float32)
    stacked = jnp.concatenate([half_real, half_imag], axis=1).astype(jnp.float32)
    surface = jnp.einsum('ntk,nku->ntu', row_table, stacked) / length
    weights = surface * surface
    displacement = (jnp.arange(LAGS, dtype=jnp.int32) - LAGS // 2).astype(jnp.float32)
    weight_sum = 1.0 + jnp.sum(weights, axis=(1, 2))
    row_shift = jnp.sum(weights * displacement[None, :, None], axis=(1, 2)) / weight_sum
    column_shift = jnp.sum(weights * displacement[None, None, :], axis=(1, 2)) / weight_sum
    return jnp.stack([offsets[0].astype(jnp.float32) + row_shift, offsets[1].astype(jnp.float32) + column_shift], axis=0)


def reference(sections, priors, row_order):
    minus_table, plus_table = dft_tables(PATCH)
    margin = HALO // 2
    padded = jnp.pad(sections, ((0, 0), (margin, HALO - margin), (margin, HALO - margin)))
    place_count = GRID_R * GRID_C
    offsets_all = jnp.transpose(priors, (2, 3, 0, 1)).reshape(place_count, 2, SECTIONS)
    positions = jnp.arange(place_count, dtype=jnp.int32)

    def one_place(inputs):
        position, offsets = inputs
        top_edge = (position // GRID_C) * STRIDE
        left_edge = (position % GRID_C) * STRIDE
        window = lax.dynamic_slice(padded, (jnp.int32(0), top_edge.astype(jnp.int32), left_edge.astype(jnp.int32)), (SECTIONS, PATCH, PATCH))
        spectra = spectra_of(window, minus_table, plus_table)
        following = jnp.concatenate([spectra[1:], spectra[:1]], axis=0)
        return flows_of(spectra, following, offsets)

    all_flows = lax.map(one_place, (positions, offsets_all))
    flow_table = jnp.transpose(all_flows.reshape(GRID_R, GRID_C, 2, SECTIONS), (2, 3, 0, 1))
    picked = flow_table[:, :, row_order, :]
    return jnp.transpose(picked, (2, 0, 1, 3)).reshape(GRID_R, 2 * SECTIONS * GRID_C)
```

```python
import math

import jax
import jax.numpy as jnp
import numpy as np
from jax import lax
from jax.experimental import pallas as pl
from jax.experimental.pallas import tpu as pltpu
from jax.sharding import PartitionSpec as P

PATCH = 512
STRIDE = 256
LAGS = 128
HALO = 256
HALF = PATCH // 2
QUARTER = PATCH // 4
KROWS = HALF + 16


def angle_of(products):
    return (products % PATCH) * (2.0 * math.pi / PATCH)


def dft_table():
    k = np.arange(HALF)[:, None]
    x = np.arange(PATCH)[None, :]
    table = np.zeros((2 * KROWS, PATCH))
    table[:HALF] = np.cos(angle_of(k * x))
    table[HALF] = np.cos(angle_of(HALF * x[0]))
    table[KROWS : KROWS + HALF] = -np.sin(angle_of(k * x))
    return table


def split_tables():
    y = np.arange(QUARTER)[:, None]
    blocks = []
    for g in range(4):
        l = 4 * np.arange(QUARTER)[None, :] + g
        c, s = np.cos(angle_of(y * l)), np.sin(angle_of(y * l))
        blocks.append(np.block([[c, -s], [s, c]]))
    return np.stack(blocks)


def lag_tables():
    lag = np.arange(2 * LAGS)[:, None] - LAGS
    l = np.concatenate([4 * np.arange(QUARTER) + g for g in range(4)])[None, :]
    k = np.arange(KROWS)[None, :]
    weight = np.where(k == 0, 1.0, np.where(k < HALF, 2.0, np.where(k == HALF, 1.0, 0.0)))
    col = (np.cos(angle_of(lag * l)), np.sin(angle_of(lag * l)))
    row_cos = np.cos(angle_of(lag * k)) * weight
    row_sin = -np.sin(angle_of(lag * k)) * weight
    row = np.concatenate([row_cos, row_sin], axis=1)
    return col[0], col[1], row


def bf16_const(value):
    return value.astype(np.float32).astype(jnp.bfloat16)


def f32_const(value):
    return bf16_const(value).astype(np.float32)


def spectrum_pair(ext, section, i, dft_ref, wg_ref, spec_ref, pq_ref, base):
    window = ext[section, pl.ds(pl.multiple_of(i * STRIDE, STRIDE), PATCH), :]
    pq_ref[...] = jnp.dot(dft_ref[...], window, preferred_element_type=jnp.float32)
    for j in range(2):
        p, q = [], []
        for t in range(4):
            lanes = slice(j * STRIDE + t * QUARTER, j * STRIDE + (t + 1) * QUARTER)
            p.append(pq_ref[:KROWS, lanes])
            q.append(pq_ref[KROWS:, lanes])
        ps, pd, qs, qd = p[0] + p[2], p[0] - p[2], q[0] + q[2], q[0] - q[2]
        pt, pu, qt, qu = p[1] + p[3], p[1] - p[3], q[1] + q[3], q[1] - q[3]
        groups = ((ps + pt, qs + qt), (pd + qu, qd - pu), (ps - pt, qs - qt), (pd - qu, qd + pu))
        for g, (real, imag) in enumerate(groups):
            left = jnp.concatenate([real.astype(jnp.bfloat16), imag.astype(jnp.bfloat16)], axis=1)
            out = jnp.dot(left, wg_ref[g], preferred_element_type=jnp.float32).astype(jnp.bfloat16)
            lo = g * QUARTER
            spec_ref[base + j, :, lo : lo + QUARTER] = out[:, :QUARTER]
            spec_ref[base + j, :, PATCH + lo : PATCH + lo + QUARTER] = out[:, QUARTER:]


def lag_rows(table, prior):
    tiles = [
        table[t, pl.ds(prior + LAGS // 2, LAGS), :].astype(jnp.bfloat16)
        for t in range(table.shape[0])
    ]
    return jnp.concatenate(tiles, axis=1)


def lane_tiles(table):
    width = -(-table.shape[1] // LAGS) * LAGS
    table = np.pad(table, ((0, 0), (0, width - table.shape[1])))
    return np.stack(np.split(table, width // LAGS, axis=1))


def pair_flow(first, second, p, q, spec_ref, colc_ref, cols_ref, row_ref):
    f32 = jnp.float32
    ar = spec_ref[first, :, :PATCH].astype(f32)
    ai = spec_ref[first, :, PATCH:].astype(f32)
    br = spec_ref[second, :, :PATCH].astype(f32)
    bi = spec_ref[second, :, PATCH:].astype(f32)
    cr = (ar * br + ai * bi).astype(jnp.bfloat16)
    ci = (ar * bi - ai * br).astype(jnp.bfloat16)
    ec = lag_rows(colc_ref, q)
    es = lag_rows(cols_ref, q)
    left = jnp.concatenate([cr, ci], axis=1)
    right = jnp.concatenate(
        [jnp.concatenate([ec, -es], axis=1), jnp.concatenate([es, ec], axis=1)], axis=0
    )
    half = lax.dot_general(
        left, right, (((1,), (1,)), ((), ())), preferred_element_type=f32
    ).astype(jnp.bfloat16)
    stacked = jnp.concatenate([half[:, :LAGS], half[:, LAGS:]], axis=0)
    rows = lag_rows(row_ref, p)[:, : 2 * KROWS]
    surface = jnp.dot(rows, stacked, preferred_element_type=f32) * (1.0 / PATCH**3)
    w = surface * surface
    da = (lax.broadcasted_iota(jnp.int32, (LAGS, LAGS), 0) - LAGS // 2).astype(f32)
    db = (lax.broadcasted_iota(jnp.int32, (1, LAGS), 1) - LAGS // 2).astype(f32)
    col_w = jnp.sum(w, axis=0, keepdims=True)
    total = 1.0 + jnp.sum(col_w, axis=1, keepdims=True)
    row_m = jnp.sum(jnp.sum(w * da, axis=0, keepdims=True), axis=1, keepdims=True)
    col_m = jnp.sum(col_w * db, axis=1, keepdims=True)
    return p.astype(f32) + row_m / total, q.astype(f32) + col_m / total


def kernel(pri_ref, ext, dft_ref, wg_ref, colc_ref, cols_ref, row_ref, out_ref, spec_ref, pq_ref):
    def spectra(n, carry):
        spectrum_pair(ext, n // 2, n % 2, dft_ref, wg_ref, spec_ref, pq_ref, n * 2)
        return carry

    lax.fori_loop(0, 6, spectra, 0)
    lane = lax.broadcasted_iota(jnp.int32, (1, LAGS), 1)

    def pairs(n, carry):
        a, b = pair_flow(
            n, n + 4, pri_ref[n], pri_ref[8 + n], spec_ref, colc_ref, cols_ref, row_ref
        )
        out_ref[pl.ds(n, 1), :] = jnp.where(lane == 0, a, b)
        return carry

    lax.fori_loop(0, 8, pairs, 0)


def with_halo(shard, sides, width):
    for axis, dim in sides:
        devices, length = (lax.axis_size(axis), shard.shape[dim])
        up = [(i, (i + 1) % devices) for i in range(devices - 1)]
        down = [(j, i) for i, j in up]
        last = lax.slice_in_dim(shard, length - width, length, axis=dim)
        first = lax.slice_in_dim(shard, 0, width, axis=dim)
        before = lax.ppermute(last, axis, up)
        after = lax.ppermute(first, axis, down)
        shard = jnp.concatenate([before, shard, after], axis=dim)
    return shard


def shifted(value, axis, steps):
    count = lax.axis_size(axis)
    pairs = [(source, (source + steps) % count) for source in range(count)]
    return lax.ppermute(value, axis, pairs)


def body(sections, priors, row_order):
    sec_count = sections.shape[0]
    per_side = sections.shape[1] // STRIDE
    place_count = per_side * per_side
    arrived = shifted(sections[:1], "gz", -1)
    extended = with_halo(
        jnp.concatenate([sections, arrived], axis=0), (("row", 1), ("col", 2)), HALO // 2
    )
    colc, cols, row = lag_tables()
    vmem = pl.BlockSpec(memory_space=pltpu.VMEM)
    flows = pl.pallas_call(
        kernel,
        out_shape=jax.ShapeDtypeStruct((8, LAGS), jnp.float32),
        in_specs=[pl.BlockSpec(memory_space=pltpu.SMEM)] + [vmem] * 6,
        out_specs=vmem,
        scratch_shapes=[
            pltpu.VMEM((12, KROWS, 2 * PATCH), jnp.bfloat16),
            pltpu.VMEM((2 * KROWS, 768), jnp.float32),
        ],
        compiler_params=pltpu.CompilerParams(vmem_limit_bytes=50 << 20),
    )(
        priors.reshape(-1),
        extended,
        bf16_const(dft_table()),
        bf16_const(split_tables()),
        f32_const(lane_tiles(colc)),
        f32_const(lane_tiles(cols)),
        f32_const(lane_tiles(row)),
    )
    flat_flows = flows[:, :2].T.reshape(1, 2 * sec_count * place_count)
    gathered = lax.all_gather(flat_flows, ("gz", "row", "col"), axis=0, tiled=True)
    size_gz = lax.axis_size("gz")
    size_row = lax.axis_size("row")
    size_col = lax.axis_size("col")
    whole_grid = gathered.reshape(size_gz, size_row, size_col, 2, sec_count, per_side, per_side)
    whole_grid = jnp.transpose(whole_grid, (3, 0, 4, 1, 5, 2, 6)).reshape(
        2, size_gz * sec_count, size_row * per_side, size_col * per_side
    )
    rows_each = row_order.shape[0] // size_row
    owned = lax.dynamic_slice_in_dim(row_order, lax.axis_index("row") * rows_each, rows_each)
    selector = (owned[:, None] == jnp.arange(row_order.shape[0], dtype=jnp.int32)[None, :]).astype(
        jnp.float32
    )
    picked = jnp.einsum("jr,csrk->jcsk", selector, whole_grid, precision=lax.Precision.HIGHEST)
    return picked.reshape(rows_each, 2 * size_gz * sec_count * size_col * per_side)


def solution(mesh):
    placed = (P("gz", "row", "col"), P(None, "gz", "row", "col"), P())
    return jax.shard_map(
        body, mesh=mesh, in_specs=placed, out_specs=P("row", None), check_vma=False
    )
```

```python
import math

import jax
import jax.numpy as jnp
import numpy as np
from jax import lax
from jax.experimental import pallas as pl
from jax.experimental.pallas import tpu as pltpu
from jax.sharding import PartitionSpec as P

PATCH = 512
STRIDE = 256
LAGS = 128
HALO = 256
HALF = PATCH // 2
QUARTER = PATCH // 4
KROWS = HALF + 16


def angle_of(products):
    return (products % PATCH) * (2.0 * math.pi / PATCH)


def dft_table():
    k = np.arange(HALF)[:, None]
    x = np.arange(PATCH)[None, :]
    table = np.zeros((2 * KROWS, PATCH))
    table[:HALF] = np.cos(angle_of(k * x))
    table[HALF] = np.cos(angle_of(HALF * x[0]))
    table[KROWS : KROWS + HALF] = -np.sin(angle_of(k * x))
    return table


def split_tables():
    y = np.arange(QUARTER)[:, None]
    blocks = []
    for g in range(4):
        l = 4 * np.arange(QUARTER)[None, :] + g
        c, s = np.cos(angle_of(y * l)), np.sin(angle_of(y * l))
        blocks.append(np.block([[c, -s], [s, c]]))
    return np.stack(blocks)


def lag_tables():
    lag = np.arange(2 * LAGS)[:, None] - LAGS
    l = np.concatenate([4 * np.arange(QUARTER) + g for g in range(4)])[None, :]
    k = np.arange(KROWS)[None, :]
    weight = np.where(k == 0, 1.0, np.where(k < HALF, 2.0, np.where(k == HALF, 1.0, 0.0)))
    col = (np.cos(angle_of(lag * l)), np.sin(angle_of(lag * l)))
    row_cos = np.cos(angle_of(lag * k)) * weight
    row_sin = -np.sin(angle_of(lag * k)) * weight
    row = np.concatenate([row_cos, row_sin], axis=1)
    return col[0], col[1], row


def bf16_const(value):
    return value.astype(np.float32).astype(jnp.bfloat16)


def f32_const(value):
    return bf16_const(value).astype(np.float32)


def spectrum_pair(ext, section, i, dft_ref, wg_ref, spec_ref, pq_ref, base):
    window = ext[section, pl.ds(pl.multiple_of(i * STRIDE, STRIDE), PATCH), :]
    pq_ref[...] = jnp.dot(dft_ref[...], window, preferred_element_type=jnp.float32)
    for j in range(2):
        p, q = [], []
        for t in range(4):
            lanes = slice(j * STRIDE + t * QUARTER, j * STRIDE + (t + 1) * QUARTER)
            p.append(pq_ref[:KROWS, lanes])
            q.append(pq_ref[KROWS:, lanes])
        ps, pd, qs, qd = p[0] + p[2], p[0] - p[2], q[0] + q[2], q[0] - q[2]
        pt, pu, qt, qu = p[1] + p[3], p[1] - p[3], q[1] + q[3], q[1] - q[3]
        groups = ((ps + pt, qs + qt), (pd + qu, qd - pu), (ps - pt, qs - qt), (pd - qu, qd + pu))
        for g, (real, imag) in enumerate(groups):
            left = jnp.concatenate([real.astype(jnp.bfloat16), imag.astype(jnp.bfloat16)], axis=1)
            out = jnp.dot(left, wg_ref[g], preferred_element_type=jnp.float32).astype(jnp.bfloat16)
            lo = g * QUARTER
            spec_ref[base + j, :, lo : lo + QUARTER] = out[:, :QUARTER]
            spec_ref[base + j, :, PATCH + lo : PATCH + lo + QUARTER] = out[:, QUARTER:]


def lag_rows(table, prior):
    tiles = [
        table[t, pl.ds(prior + LAGS // 2, LAGS), :].astype(jnp.bfloat16)
        for t in range(table.shape[0])
    ]
    return jnp.concatenate(tiles, axis=1)


def lane_tiles(table):
    width = -(-table.shape[1] // LAGS) * LAGS
    table = np.pad(table, ((0, 0), (0, width - table.shape[1])))
    return np.stack(np.split(table, width // LAGS, axis=1))


def pair_flow(first, second, p, q, spec_ref, colc_ref, cols_ref, row_ref):
    f32 = jnp.float32
    ar = spec_ref[first, :, :PATCH].astype(f32)
    ai = spec_ref[first, :, PATCH:].astype(f32)
    br = spec_ref[second, :, :PATCH].astype(f32)
    bi = spec_ref[second, :, PATCH:].astype(f32)
    cr = (ar * br + ai * bi).astype(jnp.bfloat16)
    ci = (ar * bi - ai * br).astype(jnp.bfloat16)
    ec = lag_rows(colc_ref, q)
    es = lag_rows(cols_ref, q)
    left = jnp.concatenate([cr, ci], axis=1)
    right = jnp.concatenate(
        [jnp.concatenate([ec, -es], axis=1), jnp.concatenate([es, ec], axis=1)], axis=0
    )
    half = lax.dot_general(
        left, right, (((1,), (1,)), ((), ())), preferred_element_type=f32
    ).astype(jnp.bfloat16)
    stacked = jnp.concatenate([half[:, :LAGS], half[:, LAGS:]], axis=0)
    rows = lag_rows(row_ref, p)[:, : 2 * KROWS]
    surface = jnp.dot(rows, stacked, preferred_element_type=f32) * (1.0 / PATCH**3)
    w = surface * surface
    da = (lax.broadcasted_iota(jnp.int32, (LAGS, LAGS), 0) - LAGS // 2).astype(f32)
    db = (lax.broadcasted_iota(jnp.int32, (1, LAGS), 1) - LAGS // 2).astype(f32)
    col_w = jnp.sum(w, axis=0, keepdims=True)
    total = 1.0 + jnp.sum(col_w, axis=1, keepdims=True)
    row_m = jnp.sum(jnp.sum(w * da, axis=0, keepdims=True), axis=1, keepdims=True)
    col_m = jnp.sum(col_w * db, axis=1, keepdims=True)
    return p.astype(f32) + row_m / total, q.astype(f32) + col_m / total


def make_kernel(sizes, rows_each):
    size_gz, size_row, size_col = sizes
    count = size_gz * size_row * size_col
    side = 2 * STRIDE
    margin = HALO // 2
    far = side - margin
    mesh_id = pl.DeviceIdType.MESH
    steps = [(a, b) for a in (-1, 0, 1) for b in (-1, 0, 1) if (a, b) != (0, 0)]
    halo_span = {-1: (0, margin), 0: (margin, side), 1: (margin + side, margin)}
    edge_span = {-1: (0, margin), 0: (0, side), 1: (far, margin)}
    chunks = (
        (0, side, 0, margin),
        (0, side, far, margin),
        (0, margin, margin, far - margin),
        (far, margin, margin, far - margin),
        (margin, far - margin, margin, far - margin),
    )
    needs = {(0, -1): 1, (-1, -1): 1, (1, -1): 1, (0, 1): 2, (-1, 1): 2, (1, 1): 2, (-1, 0): 3}
    needs[(1, 0)] = 4

    def kernel(
        pri_ref, order_ref, sec_hbm, dft_hbm, wg_hbm, colc_hbm, cols_hbm, row_hbm, out_ref,
        ext, dft_ref, wg_ref, colc_ref, cols_ref, row_ref, spec_ref, pq_ref, mine_ref, all_ref,
        load_sem, own_send, own_recv, next_send, next_recv, chunk_send, chunk_recv, flow_send,
        flow_recv,
    ):
        gz, row, col = lax.axis_index("gz"), lax.axis_index("row"), lax.axis_index("col")
        flat = (gz * size_row + row) * size_col + col

        def device(number):
            return (
                number // (size_row * size_col),
                (number // size_col) % size_row,
                number % size_col,
            )

        loads = [
            pltpu.make_async_copy(
                sec_hbm, ext.at[0:2, margin : margin + side, margin : margin + side],
                load_sem.at[0],
            )
        ]
        tables = (
            (dft_hbm, dft_ref), (wg_hbm, wg_ref), (colc_hbm, colc_ref), (cols_hbm, cols_ref),
            (row_hbm, row_ref),
        )
        for n, (source, target) in enumerate(tables):
            loads.append(pltpu.make_async_copy(source, target, load_sem.at[n + 1]))
        for copy in loads:
            copy.start()

        barrier = pltpu.get_barrier_semaphore()

        def greet(n, carry):
            other = (flat + n) % count
            pl.semaphore_signal(barrier, 1, device_id=device(other), device_id_type=mesh_id)
            return carry

        lax.fori_loop(1, count, greet, 0)

        def exists(step):
            a, b = step
            ok = None
            for delta, place, size in ((a, row, size_row), (b, col, size_col)):
                if delta:
                    this = place > 0 if delta < 0 else place < size - 1
                    ok = this if ok is None else jnp.logical_and(ok, this)
            return ok

        def region(step):
            (r0, rn), (c0, cn) = halo_span[step[0]], halo_span[step[1]]
            return slice(r0, r0 + rn), slice(c0, c0 + cn)

        def edge(step, offset):
            (r0, rn), (c0, cn) = edge_span[step[0]], edge_span[step[1]]
            return slice(r0 + offset, r0 + rn + offset), slice(c0 + offset, c0 + cn + offset)

        def own_copy(n):
            step = steps[n]
            back = (-step[0], -step[1])
            return pltpu.make_async_remote_copy(
                src_ref=sec_hbm.at[(slice(0, 2), *edge(step, 0))],
                dst_ref=ext.at[(slice(0, 2), *region(back))],
                send_sem=own_send.at[n], recv_sem=own_recv.at[steps.index(back)],
                device_id=(gz, row + step[0], col + step[1]), device_id_type=mesh_id,
            )

        def next_copy(n):
            step = steps[n]
            back = (-step[0], -step[1])
            return pltpu.make_async_remote_copy(
                src_ref=ext.at[(2, *edge(step, margin))],
                dst_ref=ext.at[(2, *region(back))],
                send_sem=next_send.at[n], recv_sem=next_recv.at[steps.index(back)],
                device_id=(gz, row + step[0], col + step[1]), device_id_type=mesh_id,
            )

        def own_wait(n):
            ref = ext.at[(slice(0, 2), *region(steps[n]))]
            pltpu.make_async_copy(ref, ref, own_recv.at[n]).wait()

        def next_wait(n):
            ref = ext.at[(2, *region(steps[n]))]
            pltpu.make_async_copy(ref, ref, next_recv.at[n]).wait()

        def chunk_copy(n):
            r0, rn, c0, cn = chunks[n]
            return pltpu.make_async_remote_copy(
                src_ref=sec_hbm.at[0, r0 : r0 + rn, c0 : c0 + cn],
                dst_ref=ext.at[
                    2, margin + r0 : margin + r0 + rn, margin + c0 : margin + c0 + cn
                ],
                send_sem=chunk_send.at[n], recv_sem=chunk_recv.at[n],
                device_id=((gz + size_gz - 1) % size_gz, row, col), device_id_type=mesh_id,
            )

        for n, step in enumerate(steps):
            @pl.when(jnp.logical_not(exists(step)))
            def _(step=step):
                rows, cols = region(step)
                ext[:, rows, cols] = jnp.zeros(
                    (3, rows.stop - rows.start, cols.stop - cols.start), ext.dtype
                )

        mine_ref[...] = jnp.zeros_like(mine_ref)
        pl.semaphore_wait(barrier, count - 1)
        for n in range(len(chunks)):
            chunk_copy(n).start()
        for n, step in enumerate(steps):
            @pl.when(exists(step))
            def _(n=n):
                own_copy(n).start()
        for copy in loads:
            copy.wait()
        for n, step in enumerate(steps):
            @pl.when(exists(step))
            def _(n=n):
                own_wait(n)

        def spectra(n, carry):
            spectrum_pair(ext, n // 2, n % 2, dft_ref, wg_ref, spec_ref, pq_ref, n * 2)
            return carry

        def forward(low, high):
            for n in range(low, high):
                chunk_copy(n).wait_recv()
                for m, step in enumerate(steps):
                    if needs[step] == n + 1:
                        @pl.when(exists(step))
                        def _(m=m):
                            next_copy(m).start()

        lane = lax.broadcasted_iota(jnp.int32, (1, LAGS), 1)
        sections, columns = 2 * size_gz, 2 * size_col

        def pairs(n, carry):
            a, b = pair_flow(
                n, n + 4, pri_ref[n], pri_ref[8 + n], spec_ref, colc_ref, cols_ref, row_ref
            )
            i = (n // 2) % 2
            at = (2 * gz + n // 4) * columns + 2 * col + n % 2
            mine_ref[i] = (
                mine_ref[i]
                + jnp.where(lane == at, a, 0.0)
                + jnp.where(lane == at + sections * columns, b, 0.0)
            )
            return carry

        lax.fori_loop(0, 4, spectra, 0)
        forward(0, 2)
        lax.fori_loop(0, 4, pairs, 0)
        forward(2, 5)
        for n, step in enumerate(steps):
            @pl.when(exists(step))
            def _(n=n):
                next_wait(n)
        lax.fori_loop(4, 6, spectra, 0)
        lax.fori_loop(4, 8, pairs, 0)

        total_rows = 2 * size_row
        slot = gz * size_col + col
        place = slot * total_rows + 2 * row

        def flow_copy(n):
            return pltpu.make_async_remote_copy(
                src_ref=mine_ref, dst_ref=all_ref.at[pl.ds(place, 2)],
                send_sem=flow_send, recv_sem=flow_recv,
                device_id=device((flat + n) % count), device_id_type=mesh_id,
            )

        def send(n, carry):
            flow_copy(n).start()
            return carry

        lax.fori_loop(1, count, send, 0)
        all_ref[place] = mine_ref[0]
        all_ref[place + 1] = mine_ref[1]
        for n in range(len(chunks)):
            chunk_copy(n).wait_send()
        for n, step in enumerate(steps):
            @pl.when(exists(step))
            def _(n=n):
                own_copy(n).wait_send()
                next_copy(n).wait_send()
        got = all_ref.at[pl.ds(0, 2 * (count - 1))]
        pltpu.make_async_copy(got, got, flow_recv).wait()
        for m in range(rows_each):
            wanted = order_ref[row * rows_each + m]
            value = all_ref[wanted]
            for other in range(1, size_gz * size_col):
                value = value + all_ref[other * total_rows + wanted]
            out_ref[m : m + 1, :] = value
        pltpu.make_async_copy(got, got, flow_send).wait()

    return kernel


def body(sections, priors, row_order):
    sizes = tuple(lax.axis_size(name) for name in ("gz", "row", "col"))
    count = math.prod(sizes)
    rows_each = row_order.shape[0] // sizes[1]
    width = 2 * 2 * sizes[0] * 2 * sizes[2]
    colc, cols, row = lag_tables()
    tables = (
        bf16_const(dft_table()),
        bf16_const(split_tables()),
        f32_const(lane_tiles(colc)),
        f32_const(lane_tiles(cols)),
        f32_const(lane_tiles(row)),
    )
    smem = pl.BlockSpec(memory_space=pltpu.SMEM)
    hbm = pl.BlockSpec(memory_space=pl.ANY)
    dma = pltpu.SemaphoreType.DMA
    wide = 2 * STRIDE + HALO
    flows = pl.pallas_call(
        make_kernel(sizes, rows_each),
        out_shape=jax.ShapeDtypeStruct((rows_each, LAGS), jnp.float32),
        in_specs=[smem, smem] + [hbm] * 6,
        out_specs=pl.BlockSpec(memory_space=pltpu.VMEM),
        scratch_shapes=[
            pltpu.VMEM((3, wide, wide), jnp.bfloat16),
            *[pltpu.VMEM(t.shape, t.dtype) for t in tables],
            pltpu.VMEM((12, KROWS, 2 * PATCH), jnp.bfloat16),
            pltpu.VMEM((2 * KROWS, wide), jnp.float32),
            pltpu.VMEM((2, 1, LAGS), jnp.float32),
            pltpu.VMEM((2 * count, 1, LAGS), jnp.float32),
            dma((6,)), dma((8,)), dma((8,)), dma((8,)), dma((8,)), dma((5,)), dma((5,)),
            dma(()), dma(()),
        ],
        compiler_params=pltpu.CompilerParams(
            vmem_limit_bytes=50 << 20, collective_id=0, has_side_effects=True
        ),
    )(priors.reshape(-1), row_order, sections, *tables)
    return flows[:, :width]


def solution(mesh):
    placed = (P("gz", "row", "col"), P(None, "gz", "row", "col"), P())
    return jax.shard_map(
        body, mesh=mesh, in_specs=placed, out_specs=P("row", None), check_vma=False
    )
```

```python
import math

import jax
import jax.numpy as jnp
import numpy as np
from jax import lax
from jax.experimental import pallas as pl
from jax.experimental.pallas import tpu as pltpu
from jax.sharding import PartitionSpec as P

PATCH = 512
STRIDE = 256
LAGS = 128
HALO = 256
HALF = PATCH // 2
QUARTER = PATCH // 4
KROWS = HALF + 16


def angle_of(products):
    return (products % PATCH) * (2.0 * math.pi / PATCH)


def dft_table():
    k = np.arange(HALF)[:, None]
    x = np.arange(PATCH)[None, :]
    table = np.zeros((2 * KROWS, PATCH))
    table[:HALF] = np.cos(angle_of(k * x))
    table[HALF] = np.cos(angle_of(HALF * x[0]))
    table[KROWS : KROWS + HALF] = -np.sin(angle_of(k * x))
    return table


def split_tables():
    y = np.arange(QUARTER)[:, None]
    blocks = []
    for g in range(4):
        l = 4 * np.arange(QUARTER)[None, :] + g
        c, s = np.cos(angle_of(y * l)), np.sin(angle_of(y * l))
        blocks.append(np.block([[c, -s], [s, c]]))
    return np.stack(blocks)


def lag_tables():
    lag = np.arange(2 * LAGS)[:, None] - LAGS
    l = np.concatenate([4 * np.arange(QUARTER) + g for g in range(4)])[None, :]
    k = np.arange(KROWS)[None, :]
    weight = np.where(k == 0, 1.0, np.where(k < HALF, 2.0, np.where(k == HALF, 1.0, 0.0)))
    col = (np.cos(angle_of(lag * l)), np.sin(angle_of(lag * l)))
    row_cos = np.cos(angle_of(lag * k)) * weight
    row_sin = -np.sin(angle_of(lag * k)) * weight
    row = np.concatenate([row_cos, row_sin], axis=1)
    return col[0], col[1], row


def bf16_const(value):
    return value.astype(np.float32).astype(jnp.bfloat16)


def f32_const(value):
    return bf16_const(value).astype(np.float32)


def spectrum_pair(ext, section, i, dft_ref, wg_ref, spec_ref, pq_ref, base):
    window = ext[section, pl.ds(pl.multiple_of(i * STRIDE, STRIDE), PATCH), :]
    pq_ref[...] = jnp.dot(dft_ref[...], window, preferred_element_type=jnp.float32)
    for j in range(2):
        p, q = [], []
        for t in range(4):
            lanes = slice(j * STRIDE + t * QUARTER, j * STRIDE + (t + 1) * QUARTER)
            p.append(pq_ref[:KROWS, lanes])
            q.append(pq_ref[KROWS:, lanes])
        ps, pd, qs, qd = p[0] + p[2], p[0] - p[2], q[0] + q[2], q[0] - q[2]
        pt, pu, qt, qu = p[1] + p[3], p[1] - p[3], q[1] + q[3], q[1] - q[3]
        groups = ((ps + pt, qs + qt), (pd + qu, qd - pu), (ps - pt, qs - qt), (pd - qu, qd + pu))
        for g, (real, imag) in enumerate(groups):
            left = jnp.concatenate([real.astype(jnp.bfloat16), imag.astype(jnp.bfloat16)], axis=1)
            out = jnp.dot(left, wg_ref[g], preferred_element_type=jnp.float32).astype(jnp.bfloat16)
            lo = g * QUARTER
            spec_ref[base + j, :, lo : lo + QUARTER] = out[:, :QUARTER]
            spec_ref[base + j, :, PATCH + lo : PATCH + lo + QUARTER] = out[:, QUARTER:]


def lag_rows(table, prior):
    tiles = [
        table[t, pl.ds(prior + LAGS // 2, LAGS), :].astype(jnp.bfloat16)
        for t in range(table.shape[0])
    ]
    return jnp.concatenate(tiles, axis=1)


def lane_tiles(table):
    width = -(-table.shape[1] // LAGS) * LAGS
    table = np.pad(table, ((0, 0), (0, width - table.shape[1])))
    return np.stack(np.split(table, width // LAGS, axis=1))


def pair_flow(first, second, p, q, spec_ref, colc_ref, cols_ref, row_ref):
    f32 = jnp.float32
    ar = spec_ref[first, :, :PATCH].astype(f32)
    ai = spec_ref[first, :, PATCH:].astype(f32)
    br = spec_ref[second, :, :PATCH].astype(f32)
    bi = spec_ref[second, :, PATCH:].astype(f32)
    cr = (ar * br + ai * bi).astype(jnp.bfloat16)
    ci = (ar * bi - ai * br).astype(jnp.bfloat16)
    ec = lag_rows(colc_ref, q)
    es = lag_rows(cols_ref, q)
    left = jnp.concatenate([cr, ci], axis=1)
    right = jnp.concatenate(
        [jnp.concatenate([ec, -es], axis=1), jnp.concatenate([es, ec], axis=1)], axis=0
    )
    half = lax.dot_general(
        left, right, (((1,), (1,)), ((), ())), preferred_element_type=f32
    ).astype(jnp.bfloat16)
    stacked = jnp.concatenate([half[:, :LAGS], half[:, LAGS:]], axis=0)
    rows = lag_rows(row_ref, p)[:, : 2 * KROWS]
    surface = jnp.dot(rows, stacked, preferred_element_type=f32) * (1.0 / PATCH**3)
    w = surface * surface
    da = (lax.broadcasted_iota(jnp.int32, (LAGS, LAGS), 0) - LAGS // 2).astype(f32)
    db = (lax.broadcasted_iota(jnp.int32, (1, LAGS), 1) - LAGS // 2).astype(f32)
    col_w = jnp.sum(w, axis=0, keepdims=True)
    total = 1.0 + jnp.sum(col_w, axis=1, keepdims=True)
    row_m = jnp.sum(jnp.sum(w * da, axis=0, keepdims=True), axis=1, keepdims=True)
    col_m = jnp.sum(col_w * db, axis=1, keepdims=True)
    return p.astype(f32) + row_m / total, q.astype(f32) + col_m / total


def make_kernel(sizes, rows_each):
    size_gz, size_row, size_col = sizes
    count = size_gz * size_row * size_col
    side = 2 * STRIDE
    margin = HALO // 2
    far = side - margin
    mesh_id = pl.DeviceIdType.MESH
    steps = [(a, b) for a in (-1, 0, 1) for b in (-1, 0, 1) if (a, b) != (0, 0)]
    halo_span = {-1: (0, margin), 0: (margin, side), 1: (margin + side, margin)}
    edge_span = {-1: (0, margin), 0: (0, side), 1: (far, margin)}
    chunks = (
        (0, side, 0, margin),
        (0, side, far, margin),
        (0, margin, margin, far - margin),
        (far, margin, margin, far - margin),
        (margin, far - margin, margin, far - margin),
    )
    needs = {(0, -1): 1, (-1, -1): 1, (1, -1): 1, (0, 1): 2, (-1, 1): 2, (1, 1): 2, (-1, 0): 3}
    needs[(1, 0)] = 4

    def kernel(
        pri_ref, order_ref, sec_hbm, dft_hbm, wg_hbm, colc_hbm, cols_hbm, row_hbm, out_ref,
        ext, dft_ref, wg_ref, colc_ref, cols_ref, row_ref, spec_ref, pq_ref, mine_ref, all_ref,
        load_sem, own_send, own_recv, next_send, next_recv, chunk_send, chunk_recv, flow_send,
        flow_recv,
    ):
        gz, row, col = lax.axis_index("gz"), lax.axis_index("row"), lax.axis_index("col")
        flat = (gz * size_row + row) * size_col + col

        def device(number):
            return (
                number // (size_row * size_col),
                (number // size_col) % size_row,
                number % size_col,
            )

        loads = [
            pltpu.make_async_copy(
                sec_hbm, ext.at[0:2, margin : margin + side, margin : margin + side],
                load_sem.at[0],
            )
        ]
        tables = (
            (dft_hbm, dft_ref), (wg_hbm, wg_ref), (colc_hbm, colc_ref), (cols_hbm, cols_ref),
            (row_hbm, row_ref),
        )
        for n, (source, target) in enumerate(tables):
            loads.append(pltpu.make_async_copy(source, target, load_sem.at[n + 1]))
        for copy in loads:
            copy.start()

        barrier = pltpu.get_barrier_semaphore()

        def greet(n, carry):
            other = (flat + n) % count
            pl.semaphore_signal(barrier, 1, device_id=device(other), device_id_type=mesh_id)
            return carry

        lax.fori_loop(1, count, greet, 0)

        def exists(step):
            a, b = step
            ok = None
            for delta, place, size in ((a, row, size_row), (b, col, size_col)):
                if delta:
                    this = place > 0 if delta < 0 else place < size - 1
                    ok = this if ok is None else jnp.logical_and(ok, this)
            return ok

        def region(step):
            (r0, rn), (c0, cn) = halo_span[step[0]], halo_span[step[1]]
            return slice(r0, r0 + rn), slice(c0, c0 + cn)

        def edge(step, offset):
            (r0, rn), (c0, cn) = edge_span[step[0]], edge_span[step[1]]
            return slice(r0 + offset, r0 + rn + offset), slice(c0 + offset, c0 + cn + offset)

        def own_copy(n):
            step = steps[n]
            back = (-step[0], -step[1])
            return pltpu.make_async_remote_copy(
                src_ref=sec_hbm.at[(slice(0, 2), *edge(step, 0))],
                dst_ref=ext.at[(slice(0, 2), *region(back))],
                send_sem=own_send.at[n], recv_sem=own_recv.at[steps.index(back)],
                device_id=(gz, row + step[0], col + step[1]), device_id_type=mesh_id,
            )

        def next_copy(n):
            step = steps[n]
            back = (-step[0], -step[1])
            return pltpu.make_async_remote_copy(
                src_ref=ext.at[(2, *edge(step, margin))],
                dst_ref=ext.at[(2, *region(back))],
                send_sem=next_send.at[n], recv_sem=next_recv.at[steps.index(back)],
                device_id=(gz, row + step[0], col + step[1]), device_id_type=mesh_id,
            )

        def own_wait(n):
            ref = ext.at[(slice(0, 2), *region(steps[n]))]
            pltpu.make_async_copy(ref, ref, own_recv.at[n]).wait()

        def next_wait(n):
            ref = ext.at[(2, *region(steps[n]))]
            pltpu.make_async_copy(ref, ref, next_recv.at[n]).wait()

        def chunk_copy(n):
            r0, rn, c0, cn = chunks[n]
            return pltpu.make_async_remote_copy(
                src_ref=sec_hbm.at[0, r0 : r0 + rn, c0 : c0 + cn],
                dst_ref=ext.at[
                    2, margin + r0 : margin + r0 + rn, margin + c0 : margin + c0 + cn
                ],
                send_sem=chunk_send.at[n], recv_sem=chunk_recv.at[n],
                device_id=((gz + size_gz - 1) % size_gz, row, col), device_id_type=mesh_id,
            )

        for n, step in enumerate(steps):
            @pl.when(jnp.logical_not(exists(step)))
            def _(step=step):
                rows, cols = region(step)
                ext[:, rows, cols] = jnp.zeros(
                    (3, rows.stop - rows.start, cols.stop - cols.start), ext.dtype
                )

        mine_ref[...] = jnp.zeros_like(mine_ref)
        pl.semaphore_wait(barrier, count - 1)
        for n in range(len(chunks)):
            chunk_copy(n).start()
        for n, step in enumerate(steps):
            @pl.when(exists(step))
            def _(n=n):
                own_copy(n).start()
        for copy in loads:
            copy.wait()
        for n, step in enumerate(steps):
            @pl.when(exists(step))
            def _(n=n):
                own_wait(n)

        def spectra(n, carry):
            spectrum_pair(ext, n // 2, n % 2, dft_ref, wg_ref, spec_ref, pq_ref, n * 2)
            return carry

        def forward(low, high):
            for n in range(low, high):
                chunk_copy(n).wait_recv()
                for m, step in enumerate(steps):
                    if needs[step] == n + 1:
                        @pl.when(exists(step))
                        def _(m=m):
                            next_copy(m).start()

        lane = lax.broadcasted_iota(jnp.int32, (1, LAGS), 1)
        sections, columns = 2 * size_gz, 2 * size_col

        def prior(part, n):
            return pri_ref[part, n // 4, (n // 2) % 2, n % 2]

        def pairs_static(low, high):
            values = []
            for n in range(low, high):
                a, b = pair_flow(
                    n, n + 4, prior(0, n), prior(1, n), spec_ref, colc_ref, cols_ref, row_ref
                )
                at = (2 * gz + n // 4) * columns + 2 * col + n % 2
                values.append(
                    jnp.where(lane == at, a, 0.0)
                    + jnp.where(lane == at + sections * columns, b, 0.0)
                )
            mine_ref[0] = mine_ref[0] + values[0] + values[1]
            mine_ref[1] = mine_ref[1] + values[2] + values[3]

        lax.fori_loop(0, 4, spectra, 0, unroll=2)
        forward(0, 2)
        pairs_static(0, 4)
        forward(2, 5)
        for n, step in enumerate(steps):
            @pl.when(exists(step))
            def _(n=n):
                next_wait(n)
        lax.fori_loop(4, 6, spectra, 0, unroll=2)
        pairs_static(4, 8)

        total_rows = 2 * size_row
        slot = gz * size_col + col
        place = slot * total_rows + 2 * row

        def flow_copy(n):
            return pltpu.make_async_remote_copy(
                src_ref=mine_ref, dst_ref=all_ref.at[pl.ds(place, 2)],
                send_sem=flow_send, recv_sem=flow_recv,
                device_id=device((flat + n) % count), device_id_type=mesh_id,
            )

        def send(n, carry):
            flow_copy(n).start()
            return carry

        lax.fori_loop(1, count, send, 0)
        all_ref[place] = mine_ref[0]
        all_ref[place + 1] = mine_ref[1]
        for n in range(len(chunks)):
            chunk_copy(n).wait_send()
        for n, step in enumerate(steps):
            @pl.when(exists(step))
            def _(n=n):
                own_copy(n).wait_send()
                next_copy(n).wait_send()
        got = all_ref.at[pl.ds(0, 2 * (count - 1))]
        pltpu.make_async_copy(got, got, flow_recv).wait()
        for m in range(rows_each):
            wanted = order_ref[row * rows_each + m]
            value = all_ref[wanted]
            for other in range(1, size_gz * size_col):
                value = value + all_ref[other * total_rows + wanted]
            out_ref[m : m + 1, :] = value[:, : out_ref.shape[1]]
        pltpu.make_async_copy(got, got, flow_send).wait()

    return kernel


def body(sections, priors, row_order):
    sizes = tuple(lax.axis_size(name) for name in ("gz", "row", "col"))
    count = math.prod(sizes)
    rows_each = row_order.shape[0] // sizes[1]
    width = 2 * 2 * sizes[0] * 2 * sizes[2]
    colc, cols, row = lag_tables()
    tables = (
        bf16_const(dft_table()),
        bf16_const(split_tables()),
        f32_const(lane_tiles(colc)),
        f32_const(lane_tiles(cols)),
        f32_const(lane_tiles(row)),
    )
    smem = pl.BlockSpec(memory_space=pltpu.SMEM)
    hbm = pl.BlockSpec(memory_space=pl.ANY)
    dma = pltpu.SemaphoreType.DMA
    wide = 2 * STRIDE + HALO
    flows = pl.pallas_call(
        make_kernel(sizes, rows_each),
        out_shape=jax.ShapeDtypeStruct((rows_each, width), jnp.float32),
        in_specs=[smem, smem] + [hbm] * 6,
        out_specs=pl.BlockSpec(memory_space=pltpu.VMEM),
        scratch_shapes=[
            pltpu.VMEM((3, wide, wide), jnp.bfloat16),
            *[pltpu.VMEM(t.shape, t.dtype) for t in tables],
            pltpu.VMEM((12, KROWS, 2 * PATCH), jnp.bfloat16),
            pltpu.VMEM((2 * KROWS, wide), jnp.float32),
            pltpu.VMEM((2, 1, LAGS), jnp.float32),
            pltpu.VMEM((2 * count, 1, LAGS), jnp.float32),
            dma((6,)), dma((8,)), dma((8,)), dma((8,)), dma((8,)), dma((5,)), dma((5,)),
            dma(()), dma(()),
        ],
        compiler_params=pltpu.CompilerParams(
            vmem_limit_bytes=67043328, collective_id=0, has_side_effects=True
        ),
    )(priors, row_order, sections, *tables)
    return flows


def solution(mesh):
    placed = (P("gz", "row", "col"), P(None, "gz", "row", "col"), P())
    return jax.shard_map(
        body, mesh=mesh, in_specs=placed, out_specs=P("row", None), check_vma=False
    )
```

```python
import math

import jax
import jax.numpy as jnp
import numpy as np
from jax import lax
from jax.experimental import pallas as pl
from jax.experimental.pallas import tpu as pltpu
from jax.sharding import PartitionSpec as P

PATCH = 512
STRIDE = 256
LAGS = 128
HALO = 256
HALF = PATCH // 2
QUARTER = PATCH // 4
KROWS = HALF + 16


def angle_of(products):
    return (products % PATCH) * (2.0 * math.pi / PATCH)


def dft_table():
    k = np.arange(HALF)[:, None]
    x = np.arange(PATCH)[None, :]
    table = np.zeros((2 * KROWS, PATCH))
    table[:HALF] = np.cos(angle_of(k * x))
    table[HALF] = np.cos(angle_of(HALF * x[0]))
    table[KROWS : KROWS + HALF] = -np.sin(angle_of(k * x))
    return table


def split_tables():
    y = np.arange(QUARTER)[:, None]
    blocks = []
    for g in range(4):
        l = 4 * np.arange(QUARTER)[None, :] + g
        c, s = np.cos(angle_of(y * l)), np.sin(angle_of(y * l))
        blocks.append(np.block([[c, -s], [s, c]]))
    return np.stack(blocks)


def lag_tables():
    lag = np.arange(2 * LAGS)[:, None] - LAGS
    l = np.concatenate([4 * np.arange(QUARTER) + g for g in range(4)])[None, :]
    k = np.arange(KROWS)[None, :]
    weight = np.where(k == 0, 1.0, np.where(k < HALF, 2.0, np.where(k == HALF, 1.0, 0.0)))
    col = (np.cos(angle_of(lag * l)), np.sin(angle_of(lag * l)))
    row_cos = np.cos(angle_of(lag * k)) * weight
    row_sin = -np.sin(angle_of(lag * k)) * weight
    row = np.concatenate([row_cos, row_sin], axis=1)
    return col[0], col[1], row


def bf16_const(value):
    return value.astype(np.float32).astype(jnp.bfloat16)


def f32_const(value):
    return bf16_const(value).astype(np.float32)


def first_pass(ext, section, i, dft_ref, pq_ref, slot, outer):
    rows = pl.ds(pl.multiple_of(i * STRIDE, STRIDE), PATCH)
    edge, far = HALO // 2, ext.shape[2] - HALO // 2
    if not outer:
        pq_ref[slot, :, edge:far] = jnp.dot(
            dft_ref[...], ext[section, rows, edge:far], preferred_element_type=jnp.float32
        )
        return
    window = jnp.concatenate([ext[section, rows, :edge], ext[section, rows, far:]], axis=1)
    both = jnp.dot(dft_ref[...], window, preferred_element_type=jnp.float32)
    pq_ref[slot, :, :edge] = both[:, :edge]
    pq_ref[slot, :, far:] = both[:, edge:]


def spectrum_pair(wg_ref, spec_ref, pq_ref, slot, base):
    for j in range(2):
        p, q = [], []
        for t in range(4):
            lanes = slice(j * STRIDE + t * QUARTER, j * STRIDE + (t + 1) * QUARTER)
            p.append(pq_ref[slot, :KROWS, lanes])
            q.append(pq_ref[slot, KROWS:, lanes])
        ps, pd, qs, qd = p[0] + p[2], p[0] - p[2], q[0] + q[2], q[0] - q[2]
        pt, pu, qt, qu = p[1] + p[3], p[1] - p[3], q[1] + q[3], q[1] - q[3]
        groups = ((ps + pt, qs + qt), (pd + qu, qd - pu), (ps - pt, qs - qt), (pd - qu, qd + pu))
        for g, (real, imag) in enumerate(groups):
            left = jnp.concatenate([real.astype(jnp.bfloat16), imag.astype(jnp.bfloat16)], axis=1)
            out = jnp.dot(left, wg_ref[g], preferred_element_type=jnp.float32).astype(jnp.bfloat16)
            lo = g * QUARTER
            spec_ref[base + j, :, lo : lo + QUARTER] = out[:, :QUARTER]
            spec_ref[base + j, :, PATCH + lo : PATCH + lo + QUARTER] = out[:, QUARTER:]


def lag_rows(table, prior):
    tiles = [
        table[t, pl.ds(prior + LAGS // 2, LAGS), :].astype(jnp.bfloat16)
        for t in range(table.shape[0])
    ]
    return jnp.concatenate(tiles, axis=1)


def lane_tiles(table):
    width = -(-table.shape[1] // LAGS) * LAGS
    table = np.pad(table, ((0, 0), (0, width - table.shape[1])))
    return np.stack(np.split(table, width // LAGS, axis=1))


def pair_flow(first, second, p, q, spec_ref, colc_ref, cols_ref, row_ref):
    f32 = jnp.float32
    ar = spec_ref[first, :, :PATCH].astype(f32)
    ai = spec_ref[first, :, PATCH:].astype(f32)
    br = spec_ref[second, :, :PATCH].astype(f32)
    bi = spec_ref[second, :, PATCH:].astype(f32)
    cr = (ar * br + ai * bi).astype(jnp.bfloat16)
    ci = (ar * bi - ai * br).astype(jnp.bfloat16)
    ec = lag_rows(colc_ref, q)
    es = lag_rows(cols_ref, q)
    left = jnp.concatenate([cr, ci], axis=1)
    right = jnp.concatenate(
        [jnp.concatenate([ec, -es], axis=1), jnp.concatenate([es, ec], axis=1)], axis=0
    )
    half = lax.dot_general(
        left, right, (((1,), (1,)), ((), ())), preferred_element_type=f32
    ).astype(jnp.bfloat16)
    stacked = jnp.concatenate([half[:, :LAGS], half[:, LAGS:]], axis=0)
    rows = lag_rows(row_ref, p)[:, : 2 * KROWS]
    surface = jnp.dot(rows, stacked, preferred_element_type=f32) * (1.0 / PATCH**3)
    w = surface * surface
    da = (lax.broadcasted_iota(jnp.int32, (LAGS, LAGS), 0) - LAGS // 2).astype(f32)
    db = (lax.broadcasted_iota(jnp.int32, (1, LAGS), 1) - LAGS // 2).astype(f32)
    col_w = jnp.sum(w, axis=0, keepdims=True)
    total = 1.0 + jnp.sum(col_w, axis=1, keepdims=True)
    row_m = jnp.sum(jnp.sum(w * da, axis=0, keepdims=True), axis=1, keepdims=True)
    col_m = jnp.sum(col_w * db, axis=1, keepdims=True)
    return p.astype(f32) + row_m / total, q.astype(f32) + col_m / total


def make_kernel(sizes, rows_each):
    size_gz, size_row, size_col = sizes
    count = size_gz * size_row * size_col
    side = 2 * STRIDE
    margin = HALO // 2
    far = side - margin
    mesh_id = pl.DeviceIdType.MESH
    steps = [(a, b) for a in (-1, 0, 1) for b in (-1, 0, 1) if (a, b) != (0, 0)]
    halo_span = {-1: (0, margin), 0: (margin, side), 1: (margin + side, margin)}
    edge_span = {-1: (0, margin), 0: (0, side), 1: (far, margin)}
    chunks = (
        (0, side, 0, margin),
        (0, side, far, margin),
        (0, margin, margin, far - margin),
        (far, margin, margin, far - margin),
        (margin, far - margin, margin, far - margin),
    )
    needs = {(0, -1): 1, (-1, -1): 1, (1, -1): 1, (0, 1): 2, (-1, 1): 2, (1, 1): 2, (-1, 0): 3}
    needs[(1, 0)] = 4

    def kernel(
        pri_ref, order_ref, sec_hbm, dft_hbm, wg_hbm, colc_hbm, cols_hbm, row_hbm, out_ref,
        ext, dft_ref, wg_ref, colc_ref, cols_ref, row_ref, spec_ref, pq_ref, mine_ref, all_ref,
        load_sem, own_send, own_recv, next_send, next_recv, chunk_send, chunk_recv, flow_send,
        flow_recv,
    ):
        gz, row, col = lax.axis_index("gz"), lax.axis_index("row"), lax.axis_index("col")
        flat = (gz * size_row + row) * size_col + col

        def device(number):
            return (
                number // (size_row * size_col),
                (number // size_col) % size_row,
                number % size_col,
            )

        loads = [
            pltpu.make_async_copy(
                sec_hbm, ext.at[0:2, margin : margin + side, margin : margin + side],
                load_sem.at[0],
            )
        ]
        tables = (
            (dft_hbm, dft_ref), (wg_hbm, wg_ref), (colc_hbm, colc_ref), (cols_hbm, cols_ref),
            (row_hbm, row_ref),
        )
        for n, (source, target) in enumerate(tables):
            loads.append(pltpu.make_async_copy(source, target, load_sem.at[n + 1]))
        for copy in loads:
            copy.start()

        barrier = pltpu.get_barrier_semaphore()

        def greet(n, carry):
            other = (flat + n) % count
            pl.semaphore_signal(barrier, 1, device_id=device(other), device_id_type=mesh_id)
            return carry

        lax.fori_loop(1, count, greet, 0)

        def exists(step):
            a, b = step
            ok = None
            for delta, place, size in ((a, row, size_row), (b, col, size_col)):
                if delta:
                    this = place > 0 if delta < 0 else place < size - 1
                    ok = this if ok is None else jnp.logical_and(ok, this)
            return ok

        def region(step):
            (r0, rn), (c0, cn) = halo_span[step[0]], halo_span[step[1]]
            return slice(r0, r0 + rn), slice(c0, c0 + cn)

        def edge(step, offset):
            (r0, rn), (c0, cn) = edge_span[step[0]], edge_span[step[1]]
            return slice(r0 + offset, r0 + rn + offset), slice(c0 + offset, c0 + cn + offset)

        def own_copy(n):
            step = steps[n]
            back = (-step[0], -step[1])
            return pltpu.make_async_remote_copy(
                src_ref=sec_hbm.at[(slice(0, 2), *edge(step, 0))],
                dst_ref=ext.at[(slice(0, 2), *region(back))],
                send_sem=own_send.at[n], recv_sem=own_recv.at[steps.index(back)],
                device_id=(gz, row + step[0], col + step[1]), device_id_type=mesh_id,
            )

        def next_copy(n):
            step = steps[n]
            back = (-step[0], -step[1])
            return pltpu.make_async_remote_copy(
                src_ref=ext.at[(2, *edge(step, margin))],
                dst_ref=ext.at[(2, *region(back))],
                send_sem=next_send.at[n], recv_sem=next_recv.at[steps.index(back)],
                device_id=(gz, row + step[0], col + step[1]), device_id_type=mesh_id,
            )

        def own_wait(n):
            ref = ext.at[(slice(0, 2), *region(steps[n]))]
            pltpu.make_async_copy(ref, ref, own_recv.at[n]).wait()

        def next_wait(n):
            ref = ext.at[(2, *region(steps[n]))]
            pltpu.make_async_copy(ref, ref, next_recv.at[n]).wait()

        def chunk_copy(n):
            r0, rn, c0, cn = chunks[n]
            return pltpu.make_async_remote_copy(
                src_ref=sec_hbm.at[0, r0 : r0 + rn, c0 : c0 + cn],
                dst_ref=ext.at[
                    2, margin + r0 : margin + r0 + rn, margin + c0 : margin + c0 + cn
                ],
                send_sem=chunk_send.at[n], recv_sem=chunk_recv.at[n],
                device_id=((gz + size_gz - 1) % size_gz, row, col), device_id_type=mesh_id,
            )

        def forward(low, high):
            for n in range(low, high):
                chunk_copy(n).wait_recv()
                for m, step in enumerate(steps):
                    if needs[step] == n + 1:
                        @pl.when(exists(step))
                        def _(m=m):
                            next_copy(m).start()

        def halo_waits(wait, outer):
            for n, step in enumerate(steps):
                if (step[1] != 0) == outer:
                    @pl.when(exists(step))
                    def _(n=n):
                        wait(n)

        def middle(n, carry):
            first_pass(ext, n // 2, n % 2, dft_ref, pq_ref, n % 4, False)
            return carry

        def spectra(n, carry):
            first_pass(ext, n // 2, n % 2, dft_ref, pq_ref, n % 4, True)
            spectrum_pair(wg_ref, spec_ref, pq_ref, n % 4, n * 2)
            return carry

        for n, step in enumerate(steps):
            @pl.when(jnp.logical_not(exists(step)))
            def _(step=step):
                rows, cols = region(step)
                ext[:, rows, cols] = jnp.zeros(
                    (3, rows.stop - rows.start, cols.stop - cols.start), ext.dtype
                )

        mine_ref[...] = jnp.zeros_like(mine_ref)
        pl.semaphore_wait(barrier, count - 1)
        for n in range(len(chunks)):
            chunk_copy(n).start()
        for n, step in enumerate(steps):
            @pl.when(exists(step))
            def _(n=n):
                own_copy(n).start()
        for copy in loads:
            copy.wait()
        halo_waits(own_wait, False)
        lax.fori_loop(0, 4, middle, 0, unroll=2)
        forward(0, 2)
        halo_waits(own_wait, True)

        lane = lax.broadcasted_iota(jnp.int32, (1, LAGS), 1)
        sections, columns = 2 * size_gz, 2 * size_col

        def prior(part, n):
            return pri_ref[part, n // 4, (n // 2) % 2, n % 2]

        def pairs_static(low, high):
            values = []
            for n in range(low, high):
                a, b = pair_flow(
                    n, n + 4, prior(0, n), prior(1, n), spec_ref, colc_ref, cols_ref, row_ref
                )
                at = (2 * gz + n // 4) * columns + 2 * col + n % 2
                values.append(
                    jnp.where(lane == at, a, 0.0)
                    + jnp.where(lane == at + sections * columns, b, 0.0)
                )
            mine_ref[0] = mine_ref[0] + values[0] + values[1]
            mine_ref[1] = mine_ref[1] + values[2] + values[3]

        lax.fori_loop(0, 4, spectra, 0, unroll=2)
        forward(2, 4)
        pairs_static(0, 4)
        forward(4, 5)
        halo_waits(next_wait, False)
        lax.fori_loop(4, 6, middle, 0, unroll=2)
        halo_waits(next_wait, True)
        lax.fori_loop(4, 6, spectra, 0, unroll=2)
        pairs_static(4, 8)

        total_rows = 2 * size_row
        slot = gz * size_col + col
        place = slot * total_rows + 2 * row

        def flow_copy(n):
            return pltpu.make_async_remote_copy(
                src_ref=mine_ref, dst_ref=all_ref.at[pl.ds(place, 2)],
                send_sem=flow_send, recv_sem=flow_recv,
                device_id=device((flat + n) % count), device_id_type=mesh_id,
            )

        def send(n, carry):
            flow_copy(n).start()
            return carry

        lax.fori_loop(1, count, send, 0)
        all_ref[place] = mine_ref[0]
        all_ref[place + 1] = mine_ref[1]
        for n in range(len(chunks)):
            chunk_copy(n).wait_send()
        for n, step in enumerate(steps):
            @pl.when(exists(step))
            def _(n=n):
                own_copy(n).wait_send()
                next_copy(n).wait_send()
        got = all_ref.at[pl.ds(0, 2 * (count - 1))]
        pltpu.make_async_copy(got, got, flow_recv).wait()
        for m in range(rows_each):
            wanted = order_ref[row * rows_each + m]
            value = all_ref[wanted]
            for other in range(1, size_gz * size_col):
                value = value + all_ref[other * total_rows + wanted]
            out_ref[m : m + 1, :] = value[:, : out_ref.shape[1]]
        pltpu.make_async_copy(got, got, flow_send).wait()

    return kernel


def body(sections, priors, row_order):
    sizes = tuple(lax.axis_size(name) for name in ("gz", "row", "col"))
    count = math.prod(sizes)
    rows_each = row_order.shape[0] // sizes[1]
    width = 2 * 2 * sizes[0] * 2 * sizes[2]
    colc, cols, row = lag_tables()
    tables = (
        bf16_const(dft_table()),
        bf16_const(split_tables()),
        f32_const(lane_tiles(colc)),
        f32_const(lane_tiles(cols)),
        f32_const(lane_tiles(row)),
    )
    smem = pl.BlockSpec(memory_space=pltpu.SMEM)
    hbm = pl.BlockSpec(memory_space=pl.ANY)
    dma = pltpu.SemaphoreType.DMA
    wide = 2 * STRIDE + HALO
    flows = pl.pallas_call(
        make_kernel(sizes, rows_each),
        out_shape=jax.ShapeDtypeStruct((rows_each, width), jnp.float32),
        in_specs=[smem, smem] + [hbm] * 6,
        out_specs=pl.BlockSpec(memory_space=pltpu.VMEM),
        scratch_shapes=[
            pltpu.VMEM((3, wide, wide), jnp.bfloat16),
            *[pltpu.VMEM(t.shape, t.dtype) for t in tables],
            pltpu.VMEM((12, KROWS, 2 * PATCH), jnp.bfloat16),
            pltpu.VMEM((4, 2 * KROWS, wide), jnp.float32),
            pltpu.VMEM((2, 1, LAGS), jnp.float32),
            pltpu.VMEM((2 * count, 1, LAGS), jnp.float32),
            dma((6,)), dma((8,)), dma((8,)), dma((8,)), dma((8,)), dma((5,)), dma((5,)),
            dma(()), dma(()),
        ],
        compiler_params=pltpu.CompilerParams(
            vmem_limit_bytes=67043328, collective_id=0, has_side_effects=True
        ),
    )(priors, row_order, sections, *tables)
    return flows


def solution(mesh):
    placed = (P("gz", "row", "col"), P(None, "gz", "row", "col"), P())
    return jax.shard_map(
        body, mesh=mesh, in_specs=placed, out_specs=P("row", None), check_vma=False
    )
```
